32 devices in a mesh: groups: 2 (over y), tensor: 4 (over z), section: 4 (over x, core).
Axes of the slice: x: 2, y: 2, z: 4, core: 2. Of those that a mesh axis runs over, the one named last changes fastest.
Arguments:
- hidden: bfloat16 [16, 8192], P('groups', 'tensor'), parts along dimension 0, may hold values from -6 to 6
- norm_gain: bfloat16 [4, 8192], P('section'), may hold values from 0.5 to 1.5
- query_weight: bfloat16 [4, 8192, 512], P('section', None, 'tensor'), may hold values from -0.0625 to 0.0625
- query_bias: bfloat16 [4, 512], P('section', 'tensor'), may hold values from -10 to 10
- kv_weight: bfloat16 [4, 8192, 1024], P('section', None, 'tensor'), may hold values from -0.0625 to 0.0625
- out_weight: bfloat16 [4, 512, 8192], P('section', None, 'tensor'), may hold values from -0.25 to 0.25
- kv_pool: bfloat16 [4, 48, 16, 1024], P('section', ('groups', 'tensor')), parts along dimension 1, may hold values from -8 to 8
- page_table: int32 [16, 4], P(('groups', 'tensor')), parts along dimension 0, may hold values from 0 to 23, as said below
- context_len: int32 [16], P(('groups', 'tensor')), parts along dimension 0, may hold values from 33 to 64, as said below
Outputs:
- result: bfloat16 [16, 8192], P(('groups', 'section'), 'tensor'), parts along dimension 0
The draws below stay inside these ranges and needn't reach their ends.
There are 2 independent parts, one for each index of `groups`. The reference program is written for one: setup_inputs(seed, part) draws one part's arguments, and reference() takes and returns one part's arrays. A program takes and returns all parts, laid end to end along the dimension named above; an argument that names none is the same for every part. Nothing has to cross between parts.
Inputs may be any that keep to these rules, and one draw needn't show every extreme that they name: `page_table`: sample r belongs to block k = r // 2; its 4 pages lie in k * 6 to (k + 1) * 6 - 1. The first 2 pages are the same for all samples of a block, every other page belongs to one sample only. `context_len`: some sample has 64 cached tokens.
All inputs are finite; a program needn't handle non-finite values.
Results may differ from the reference program's by a relative error of at most 0.018.
Values may be sent and summed in bfloat16 or wider, within the bound.
A program may use at most 64 MiB of HBM per device.

```python
import jax
import jax.numpy as jnp
from jax import lax

D = 8192
HD = 128
HEADS = 4
KVH = 4
LAYERS = 4
ROW_DEV = 2
ROWS = 8
PAGE_LEN = 16
BLOCKS = 4
PREFIX_BLOCKS = 2
CTX = 64
POOL_DEV = 6
PAGES = 24
N_TENSOR = 4


def device_order(sub_key):
    return jax.random.permutation(sub_key, POOL_DEV).astype(jnp.int32)


def draw_page_table(key, part):
    orders = jax.vmap(device_order)(jax.random.split(jax.random.fold_in(key, 11), N_TENSOR))
    shared = jnp.broadcast_to(orders[:, None, :PREFIX_BLOCKS], (N_TENSOR, ROW_DEV, PREFIX_BLOCKS))
    private = orders[:, PREFIX_BLOCKS:].reshape(N_TENSOR, ROW_DEV, BLOCKS - PREFIX_BLOCKS)
    offsets = (jnp.arange(N_TENSOR, dtype=jnp.int32) * POOL_DEV)[:, None, None]
    table = jnp.concatenate([shared, private], axis=2) + offsets
    return table.reshape(ROWS, BLOCKS).astype(jnp.int32)


def draw_context_len(key, part):
    lowest = PREFIX_BLOCKS * PAGE_LEN + 1
    highest = BLOCKS * PAGE_LEN
    drawn = jax.random.randint(jax.random.fold_in(key, 23), (ROWS,), lowest, highest + 1, dtype=jnp.int32)
    marked = jax.random.randint(jax.random.fold_in(key, 29), (), 0, ROWS, dtype=jnp.int32)
    return jnp.where(jnp.arange(ROWS, dtype=jnp.int32) == marked, highest, drawn).astype(jnp.int32)


def draw_kv_pool(key, part):
    shape = (LAYERS, PAGES, PAGE_LEN, 2 * KVH * HD)
    base = jnp.clip(jax.random.normal(jax.random.fold_in(key, 31), shape, jnp.float32), -6.0, 6.0)
    return base.astype(jnp.bfloat16)


def draw_query_bias(key, part):
    shape = (LAYERS, HEADS * HD)
    base = jnp.clip(jax.random.normal(jax.random.fold_in(key, 43), shape, jnp.float32), -4.0, 4.0)
    return base.astype(jnp.bfloat16)


def level_of(rng, extent, shards, low, high):
    level, own = 1.0, jax.random.fold_in(rng, 6)
    for dim, parts in shards:
        steps = jnp.exp(jax.random.uniform(jax.random.fold_in(own, dim), (parts,), jnp.float32, low / len(shards), high / len(shards)))
        level = level * jnp.repeat(steps, extent[dim] // parts).reshape([-1 if axis == dim else 1 for axis in range(len(extent))])
    return level


def normal_values(key, extent, width, most, cuts=(), kind=jnp.bfloat16):
    level = level_of(key, extent, cuts, -0.22, 0.18) if cuts else 1.0
    values = jax.random.normal(key, extent, jnp.float32) * width * level
    return jnp.minimum(jnp.maximum(values, -most), most).astype(kind)


def setup_inputs(seed: int = 0, part: int = 0) -> dict:
    arg_keys = jax.random.split(jax.random.key(seed), 10)
    part_splits = jax.random.split(jax.random.fold_in(arg_keys[9], part), 10)
    return {
        "hidden": normal_values(part_splits[0], (ROWS, D), 1.0, 6.0, ((1, 4),)),
        "norm_gain": jnp.clip(1.0 + 0.1 * jax.random.normal(arg_keys[1], (LAYERS, D), jnp.float32), 0.5, 1.5).astype(jnp.bfloat16),
        "query_weight": normal_values(arg_keys[2], (LAYERS, D, HEADS * HD), D ** -0.5, 0.0625, ((0, 4), (2, 4))),
        "query_bias": draw_query_bias(jax.random.fold_in(arg_keys[9], 71), part),
        "kv_weight": normal_values(arg_keys[4], (LAYERS, D, 2 * KVH * HD), D ** -0.5, 0.0625, ((0, 4), (2, 4))),
        "out_weight": normal_values(arg_keys[5], (LAYERS, HEADS * HD, D), (HEADS * HD) ** -0.5, 0.25, ((0, 4), (2, 4))),
        "kv_pool": draw_kv_pool(jax.random.fold_in(jax.random.fold_in(arg_keys[9], part), 71), part),
        "page_table": draw_page_table(jax.random.fold_in(jax.random.fold_in(arg_keys[9], part), 71), part),
        "context_len": draw_context_len(jax.random.fold_in(jax.random.fold_in(arg_keys[9], part), 71), part),
    }


epsilon = 1e-06
rope_base = 1000000.0

def rotate(values, position):
    head_size = values.shape[-1]
    half_size = head_size // 2
    frequency = rope_base ** (-(jnp.arange(half_size, dtype=jnp.float32) * 2.0) / head_size)
    angles = position.astype(jnp.float32)[:, None] * frequency[None, :]
    cosine = jnp.cos(angles)[:, None, :]
    sine_part = jnp.sin(angles)[:, None, :]
    front_half = values[..., :half_size]
    back_half = values[..., half_size:]
    return jnp.concatenate([front_half * cosine - back_half * sine_part, back_half * cosine + front_half * sine_part], axis=-1)

def attend(queries, key_new, value_new, cached, position):
    row_count, head_count, head_size = queries.shape
    kv_heads = key_new.shape[1]
    group_size = head_count // kv_heads
    span_len = cached.shape[1]
    keys_all = cached[:, :, :kv_heads * head_size].reshape(row_count, span_len, kv_heads, head_size).astype(jnp.float32)
    values_all = cached[:, :, kv_heads * head_size:].reshape(row_count, span_len, kv_heads, head_size).astype(jnp.float32)
    grouped = queries.reshape(row_count, kv_heads, group_size, head_size).astype(jnp.float32)
    scaling = head_size ** (-0.5)
    scores = jnp.einsum('rkgd,rskd->rkgs', grouped, keys_all) * scaling
    own_score = jnp.einsum('rkgd,rkd->rkg', grouped, key_new.astype(jnp.float32)) * scaling
    usable = (jnp.arange(span_len, dtype=jnp.int32)[None, :] < position[:, None])[:, None, None, :]
    row_max = jnp.maximum(lax.optimization_barrier(jnp.max(jnp.where(usable, scores, -1e+30), axis=-1)), own_score)
    weights = jnp.where(usable, jnp.exp(scores - row_max[..., None]), 0.0)
    own_weight = jnp.exp(own_score - row_max)
    denominator = lax.optimization_barrier(jnp.sum(weights, axis=-1)) + own_weight
    weights = (weights / denominator[..., None]).astype(jnp.bfloat16)
    own_weight = (own_weight / denominator).astype(jnp.bfloat16)
    mixture = jnp.einsum('rkgs,rskd->rkgd', weights.astype(jnp.float32), values_all)
    mixture = mixture + own_weight.astype(jnp.float32)[..., None] * value_new.astype(jnp.float32)[:, :, None, :]
    return mixture.reshape(row_count, head_count * head_size).astype(jnp.bfloat16)

def reference(hidden, norm_gain, query_weight, query_bias, kv_weight, out_weight, kv_pool, page_table, context_len):
    stream = hidden
    for layer_index in range(LAYERS):
        wide_rows = stream.astype(jnp.float32)
        mean_sq = lax.optimization_barrier(jnp.mean(wide_rows * wide_rows, axis=1, keepdims=True))
        normed = (wide_rows * lax.rsqrt(mean_sq + epsilon) * norm_gain[layer_index].astype(jnp.float32)).astype(jnp.bfloat16)
        queries = (jnp.dot(normed, query_weight[layer_index], preferred_element_type=jnp.float32) + query_bias[layer_index].astype(jnp.float32)).astype(jnp.bfloat16)
        fresh_kv = jnp.dot(normed, kv_weight[layer_index], preferred_element_type=jnp.float32).astype(jnp.bfloat16)
        cached = kv_pool[layer_index][page_table].reshape(ROWS, CTX, 2 * KVH * HD)
        rotated = rotate(queries.reshape(ROWS, HEADS, HD).astype(jnp.float32), context_len).astype(jnp.bfloat16)
        key_new = rotate(fresh_kv[:, :KVH * HD].reshape(ROWS, KVH, HD).astype(jnp.float32), context_len).astype(jnp.bfloat16)
        value_new = fresh_kv[:, KVH * HD:].reshape(ROWS, KVH, HD)
        mixture = attend(rotated, key_new, value_new, cached, context_len)
        stream = (wide_rows + jnp.dot(mixture, out_weight[layer_index], preferred_element_type=jnp.float32)).astype(jnp.bfloat16)
    return stream
```

```python
import functools

import jax
import jax.numpy as jnp
from jax import lax
from jax.experimental import pallas as pl
from jax.experimental.pallas import tpu as pltpu
from jax.sharding import PartitionSpec as P

HD = 128
KVH = 4


epsilon = 1e-06
rope_base = 1000000.0


def shifted(value, axis, steps):
    count = lax.axis_size(axis)
    initial, last = (max(0, -steps), min(count, count - steps))
    return lax.ppermute(value, axis, [(source, source + steps) for source in range(initial, last)])


def rotate(values, position):
    head_size = values.shape[-1]
    half_size = head_size // 2
    frequency = rope_base ** (-(jnp.arange(half_size, dtype=jnp.float32) * 2.0) / head_size)
    angles = position.astype(jnp.float32)[:, None] * frequency[None, :]
    cosine = jnp.cos(angles)[:, None, :]
    sine_part = jnp.sin(angles)[:, None, :]
    front_half = values[..., :half_size]
    back_half = values[..., half_size:]
    return jnp.concatenate(
        [front_half * cosine - back_half * sine_part, back_half * cosine + front_half * sine_part],
        axis=-1,
    )


def attend(queries, key_new, value_new, cached, position):
    row_count, head_count, head_size = queries.shape
    kv_heads = key_new.shape[1]
    group_size = head_count // kv_heads
    span_len = cached.shape[1]
    keys_all = cached[:, :, : kv_heads * head_size].reshape(
        row_count, span_len, kv_heads, head_size
    )
    values_all = cached[:, :, kv_heads * head_size :].reshape(
        row_count, span_len, kv_heads, head_size
    )
    grouped = queries.reshape(row_count, kv_heads, group_size, head_size)
    scaling = head_size ** (-0.5)
    scores = (
        jnp.einsum("rkgd,rskd->rkgs", grouped, keys_all, preferred_element_type=jnp.float32)
        * scaling
    )
    own_score = (
        jnp.einsum("rkgd,rkd->rkg", grouped, key_new, preferred_element_type=jnp.float32) * scaling
    )
    usable = (jnp.arange(span_len, dtype=jnp.int32)[None, :] < position[:, None])[:, None, None, :]
    row_max = jnp.maximum(jnp.max(jnp.where(usable, scores, -1e30), axis=-1), own_score)
    weights = jnp.where(usable, jnp.exp(scores - row_max[..., None]), 0.0)
    own_weight = jnp.exp(own_score - row_max)
    denominator = jnp.sum(weights, axis=-1) + own_weight
    weights = (weights / denominator[..., None]).astype(jnp.bfloat16)
    own_weight = (own_weight / denominator).astype(jnp.bfloat16)
    mixture = jnp.einsum("rkgs,rskd->rkgd", weights, values_all, preferred_element_type=jnp.float32)
    mixture = (
        mixture
        + own_weight.astype(jnp.float32)[..., None] * value_new.astype(jnp.float32)[:, :, None, :]
    )
    return mixture.reshape(row_count, head_count * head_size).astype(jnp.bfloat16)


def shards(
    hidden,
    norm_gain,
    query_weight,
    query_bias,
    kv_weight,
    out_weight,
    kv_pool,
    page_table,
    context_len,
):
    slot_count = lax.axis_size("tensor")
    section_count = lax.axis_size("section")
    section_id = lax.axis_index("section")
    tensor_id = lax.axis_index("tensor")
    row_total, width_dev = hidden.shape
    row_dev = row_total // slot_count
    pool_pages = kv_pool.shape[1]
    gain_row = norm_gain[0].astype(jnp.float32)
    query_proj = query_weight[0]
    bias_row = query_bias[0].astype(jnp.float32)
    kv_proj = kv_weight[0]
    out_proj = out_weight[0]
    pool_layer = kv_pool[0]
    local_pages = page_table - tensor_id * pool_pages
    pieces = 1
    per_piece = row_dev // pieces
    tick_count = section_count + pieces - 1
    is_first = section_id == 0
    finished = [None] * pieces
    carried = jnp.zeros((slot_count * per_piece, width_dev), jnp.bfloat16)
    for tick_index in range(tick_count):
        if tick_index < pieces:
            blocks = hidden.reshape(slot_count, row_dev, hidden.shape[1])
            carried = jnp.where(
                is_first, blocks.reshape(slot_count * per_piece, hidden.shape[1]), carried
            )
        whole = lax.all_gather(carried, "tensor", axis=1, tiled=True)
        wide_rows = whole.astype(jnp.float32)
        mean_sq = jnp.mean(wide_rows * wide_rows, axis=1, keepdims=True)
        normed = (wide_rows * lax.rsqrt(mean_sq + epsilon) * gain_row).astype(jnp.bfloat16)
        queries = (
            jnp.dot(normed, query_proj, preferred_element_type=jnp.float32) + bias_row
        ).astype(jnp.bfloat16)
        fresh_kv = jnp.dot(normed, kv_proj, preferred_element_type=jnp.float32).astype(jnp.bfloat16)
        query_rows = lax.all_to_all(queries, "tensor", split_axis=0, concat_axis=1, tiled=True)
        fresh_rows = lax.all_to_all(fresh_kv, "tensor", split_axis=0, concat_axis=1, tiled=True)
        cached = pool_layer[local_pages].reshape(per_piece, -1, pool_layer.shape[-1])
        rotated = rotate(
            query_rows.reshape(per_piece, -1, HD).astype(jnp.float32), context_len
        ).astype(jnp.bfloat16)
        key_new = rotate(
            fresh_rows[:, : KVH * HD].reshape(per_piece, KVH, HD).astype(jnp.float32), context_len
        ).astype(jnp.bfloat16)
        value_new = fresh_rows[:, KVH * HD :].reshape(per_piece, KVH, HD)
        mixture = attend(rotated, key_new, value_new, cached, context_len)
        carried = (
            carried.astype(jnp.float32)
            + jnp.dot(
                lax.all_gather(mixture, "tensor", axis=0, tiled=True),
                out_proj,
                preferred_element_type=jnp.float32,
            )
        ).astype(jnp.bfloat16)
        if tick_index >= section_count - 1:
            finished[tick_index - section_count + 1] = carried
        if tick_index < tick_count - 1:
            carried = shifted(carried, "section", 1)
    stacked = jnp.concatenate(
        [done_part.reshape(slot_count, per_piece, width_dev) for done_part in finished], axis=1
    )
    result = stacked.reshape(row_total, width_dev)
    is_last = section_id == section_count - 1
    outgoing = jnp.where(is_last, result, jnp.zeros_like(result))[None]
    spread = lax.all_to_all(outgoing, "section", split_axis=1, concat_axis=0, tiled=True)
    return spread[section_count - 1]


MESH = pl.DeviceIdType.MESH
ANY = pl.BlockSpec(memory_space=pl.ANY)
VMEM = pl.BlockSpec(memory_space=pltpu.VMEM)
SMEM = pl.BlockSpec(memory_space=pltpu.SMEM)


def fused(
    slots,
    sections,
    hidden,
    gain,
    wq,
    bias,
    wkv,
    wo,
    pool,
    table,
    lens,
    out,
    wq_v,
    wkv_v,
    wo_v,
    stream,
    keys,
    values,
    meta,
    counts,
    cos_v,
    sin_v,
    fresh,
    parts,
    sent,
    fin,
    fin_in,
    w_sem,
    pool_sem,
    st_send,
    st_recv,
    nx_send,
    key_send,
    key_recv,
    val_send,
    val_recv,
    meta_send,
    meta_recv,
    fresh_send,
    fresh_recv,
    part_send,
    part_recv,
    fin_send,
    fin_recv,
):
    f32, bf16 = jnp.float32, jnp.bfloat16
    me = lax.axis_index("tensor")
    sec = lax.axis_index("section")
    rows, width = hidden.shape
    row_dev, blocks = table.shape
    pages, page_len = pool.shape[1], pool.shape[2]
    span = pages * page_len
    span_pad = keys.shape[1] * page_len
    kv_cols = wkv.shape[2]
    kv_half = KVH * HD
    group = slots // KVH
    near = sorted(range(slots), key=lambda d: min(d, slots - d))
    others = near[1:]
    far = near[::-1]

    def peer(d):
        return lax.rem(me + d, slots)

    def chunk(ref, src):
        return ref.at[pl.ds(pl.multiple_of(src * width, width), width)]

    def weight_copies(src):
        return (
            pltpu.make_async_copy(chunk(wq.at[0], src), chunk(wq_v, src), w_sem.at[0, src]),
            pltpu.make_async_copy(chunk(wkv.at[0], src), chunk(wkv_v, src), w_sem.at[1, src]),
        )

    def remote(src, dst, send, recv, slot, section):
        return pltpu.make_async_remote_copy(
            src_ref=src,
            dst_ref=dst,
            send_sem=send,
            recv_sem=recv,
            device_id={"tensor": slot, "section": section},
            device_id_type=MESH,
        )

    for d in near:
        for copy in weight_copies(peer(d)):
            copy.start()
    wo_copy = pltpu.make_async_copy(wo.at[0], wo_v, w_sem.at[2, 0])
    wo_copy.start()

    barrier = pltpu.get_barrier_semaphore()
    for d in range(slots):
        for e in range(sections):
            if d or e:
                pl.semaphore_signal(
                    barrier,
                    inc=1,
                    device_id={"tensor": peer(d), "section": lax.rem(sec + e, sections)},
                    device_id_type=MESH,
                )

    lane = lax.broadcasted_iota(jnp.int32, (row_dev, span_pad), 1)
    row = lax.broadcasted_iota(jnp.int32, (row_dev, span_pad), 0)
    row_c = lax.broadcasted_iota(jnp.int32, (row_dev, HD), 0)
    count = jnp.zeros((row_dev, span_pad), f32)
    length = jnp.zeros((row_dev, HD), f32)
    for r in range(row_dev):
        for b in range(blocks):
            off = lane - (table[r, b] - me * pages) * page_len
            used = (off >= 0) & (off < page_len) & (off + b * page_len < lens[r]) & (row == r)
            count += jnp.where(used, 1.0, 0.0)
        length = jnp.where(row_c == r, lens[r].astype(f32), length)
    meta[me, :, :span_pad] = count
    meta[me, :, span_pad:] = length
    for ref in (keys, values):
        if span_pad > span:
            ref[:, pages:] = jnp.zeros((slots, span_pad // page_len - pages, page_len, HD), bf16)

    pl.semaphore_wait(barrier, slots * sections - 1)

    @pl.when(sec == 0)
    def _():
        for d in far[:-1]:
            remote(hidden, stream.at[me], st_send.at[d], st_recv.at[me], peer(d), sec).start()
        stream[me] = hidden[...]

    def pool_part(slot, base):
        first = pl.multiple_of(base + (slot // group) * HD, HD)
        return pool.at[0, :, :, pl.ds(first, HD)]

    meta_copies, pool_copies = [], []
    for d in others:
        slot = peer(d)
        meta_copies.append(
            remote(meta.at[me], meta.at[me], meta_send.at[d], meta_recv.at[me], slot, sec)
        )
        pool_copies.append(
            remote(
                pool_part(slot, 0),
                keys.at[me, pl.ds(0, pages)],
                key_send.at[d],
                key_recv.at[me],
                slot,
                sec,
            )
        )
        pool_copies.append(
            remote(
                pool_part(slot, kv_half),
                values.at[me, pl.ds(0, pages)],
                val_send.at[d],
                val_recv.at[me],
                slot,
                sec,
            )
        )
    own_pool = [
        pltpu.make_async_copy(pool_part(me, 0), keys.at[me, pl.ds(0, pages)], pool_sem.at[0]),
        pltpu.make_async_copy(
            pool_part(me, kv_half), values.at[me, pl.ds(0, pages)], pool_sem.at[1]
        ),
    ]
    for copy in meta_copies + pool_copies + own_pool:
        copy.start()

    def arrived(dst, recv):
        remote(dst, dst, fin_send.at[0], recv, me, lax.rem(sec + 1, sections)).wait_recv()

    for d in others:
        src = peer(d)
        arrived(meta.at[src], meta_recv.at[src])
    counts[...] = jnp.zeros(counts.shape, f32)
    for t in range(slots):
        lines = slice(t * row_dev, (t + 1) * row_dev)
        counts[lines, t * span_pad : (t + 1) * span_pad] = meta[t, :, :span_pad]
        cos_v[lines, :] = meta[t, :, span_pad:]
    spot = lax.broadcasted_iota(jnp.int32, (rows, HD), 1)
    half = HD // 2
    pair = jnp.where(spot < half, spot, spot - half).astype(f32)
    frequency = jnp.exp(pair * (-2.0 / HD) * jnp.log(jnp.full((rows, HD), rope_base, f32)))
    angle = cos_v[...] * frequency
    cosine = jnp.cos(angle)
    sine = jnp.sin(angle) * jnp.where(spot < half, -1.0, 1.0)
    cos_v[...] = cosine
    sin_v[...] = sine

    def rope(x):
        x = x.astype(f32)
        return (x * cos_v[...] + pltpu.roll(x, half, 1) * sin_v[...]).astype(bf16)

    square = jnp.zeros((rows, 1), f32)
    q_sum = jnp.zeros((rows, HD), f32)
    kv_sum = jnp.zeros((rows, kv_cols), f32)
    for d in near:
        src = peer(d)
        for copy in weight_copies(src):
            copy.wait()
        if d == 0:

            @pl.when(sec > 0)
            def _():
                arrived(stream.at[me], st_recv.at[me])

        else:
            arrived(stream.at[src], st_recv.at[src])
        start = pl.multiple_of(src * width, width)
        x = stream[src].astype(f32)
        square += jnp.sum(x * x, axis=1, keepdims=True)
        scaled = (x * gain[:, pl.ds(start, width)].astype(f32)).astype(bf16)
        q_sum += jnp.dot(scaled, wq_v[pl.ds(start, width), :], preferred_element_type=f32)
        kv_sum += jnp.dot(scaled, wkv_v[pl.ds(start, width), :], preferred_element_type=f32)
    inverse = lax.rsqrt(square * (1.0 / (slots * width)) + epsilon)
    query = rope((q_sum * inverse + bias[...].astype(f32)).astype(bf16))
    kv_new = (kv_sum * inverse).astype(bf16)
    fresh[me, :, :HD] = query
    for j in range(kv_cols // HD):
        piece = kv_new[:, j * HD : (j + 1) * HD]
        is_key = me * kv_cols + j * HD < kv_half
        fresh[me, :, (j + 1) * HD : (j + 2) * HD] = jnp.where(
            is_key, rope(piece).astype(f32), piece.astype(f32)
        ).astype(bf16)
    fresh_copies = [
        remote(fresh.at[me], fresh.at[me], fresh_send.at[d], fresh_recv.at[me], peer(d), sec)
        for d in far[:-1]
    ]
    for copy in fresh_copies:
        copy.start()

    for copy in own_pool:
        copy.wait()
    for d in others:
        src = peer(d)
        arrived(keys.at[src, pl.ds(0, pages)], key_recv.at[src])
        arrived(values.at[src, pl.ds(0, pages)], val_recv.at[src])
    scaling = HD**-0.5
    times = counts[...]
    scores = (
        lax.dot_general(
            query,
            keys[...].reshape(slots * span_pad, HD),
            (((1,), (1,)), ((), ())),
            preferred_element_type=f32,
        )
        * scaling
    )
    top = jnp.max(jnp.where(times > 0, scores, -1e30), axis=1, keepdims=True)
    weights = jnp.where(times > 0, times * jnp.exp(scores - top), 0.0)
    total = jnp.sum(weights, axis=1, keepdims=True)
    mixed = jnp.dot(
        weights.astype(bf16),
        values[...].reshape(slots * span_pad, HD),
        preferred_element_type=f32,
    )
    parts[me, :, :HD] = mixed / total
    parts[me, :, HD:] = jnp.broadcast_to(top + jnp.log(total), (rows, HD))
    part_copies = [
        remote(parts.at[me], parts.at[me], part_send.at[d], part_recv.at[me], peer(d), sec)
        for d in far[:-1]
    ]
    for copy in part_copies:
        copy.start()

    for d in others:
        src = peer(d)
        arrived(fresh.at[src], fresh_recv.at[src])

    def fresh_head(column):
        first = HD + column % kv_cols
        return fresh[column // kv_cols, :, first : first + HD].astype(f32)

    own = []
    for h in range(slots):
        key = fresh_head((h // group) * HD)
        own.append(
            jnp.sum(fresh[h, :, :HD].astype(f32) * key, axis=1, keepdims=True) * scaling
        )
    wo_copy.wait()
    for d in others:
        src = peer(d)
        arrived(parts.at[src], part_recv.at[src])
    mixture = []
    for h in range(slots):
        share = 1.0 / (1.0 + jnp.exp(parts[h, :, HD:] - own[h]))
        value = fresh_head(kv_half + (h // group) * HD)
        mixture.append((parts[h, :, :HD] * (1.0 - share) + value * share).astype(bf16))
    mixture = jnp.concatenate(mixture, axis=1)
    new = (
        stream[me].astype(f32) + jnp.dot(mixture, wo_v[...], preferred_element_type=f32)
    ).astype(bf16)

    def next_copies():
        return [
            remote(sent, stream.at[me], nx_send.at[d], st_recv.at[me], peer(d), sec + 1)
            for d in far
        ]

    def fin_copy(j):
        return remote(fin.at[j], fin_in, fin_send.at[j], fin_recv, me, j)

    last = sections - 1

    @pl.when(sec < last)
    def _():
        sent[...] = new
        for copy in next_copies():
            copy.start()
        arrived(fin_in, fin_recv)
        out[...] = fin_in[...]
        for copy in next_copies():
            copy.wait_send()

    @pl.when(sec == last)
    def _():
        out_rows = rows // sections
        wide = new.astype(f32)
        for j in range(last):
            fin[j] = wide[j * out_rows : (j + 1) * out_rows].astype(bf16)
            fin_copy(j).start()
        out[...] = wide[last * out_rows :].astype(bf16)
        for j in range(last):
            fin_copy(j).wait_send()

    @pl.when(sec == 0)
    def _():
        for d in others:
            remote(hidden, stream.at[me], st_send.at[d], st_recv.at[me], peer(d), sec).wait_send()

    for copy in meta_copies + pool_copies + fresh_copies + part_copies:
        copy.wait_send()


def fused_shards(slots, sections, *args):
    hidden, gain, wq, bias, wkv, wo, pool, table, lens = args
    rows, width = hidden.shape
    row_dev = table.shape[0]
    pages, page_len = pool.shape[1:3]
    span_pad = -(-pages * page_len // HD) * HD
    pages_pad = span_pad // page_len
    kv_cols = wkv.shape[2]
    bf16, f32 = jnp.bfloat16, jnp.float32
    dma = pltpu.SemaphoreType.DMA
    each = dma((slots,))
    return pl.pallas_call(
        functools.partial(fused, slots, sections),
        out_shape=jax.ShapeDtypeStruct((rows // sections, width), bf16),
        in_specs=[VMEM, VMEM, ANY, VMEM, ANY, ANY, ANY, SMEM, SMEM],
        out_specs=VMEM,
        scratch_shapes=[
            pltpu.VMEM(wq.shape[1:], bf16),
            pltpu.VMEM(wkv.shape[1:], bf16),
            pltpu.VMEM(wo.shape[1:], bf16),
            pltpu.VMEM((slots, rows, width), bf16),
            pltpu.VMEM((slots, pages_pad, page_len, HD), bf16),
            pltpu.VMEM((slots, pages_pad, page_len, HD), bf16),
            pltpu.VMEM((slots, row_dev, span_pad + HD), f32),
            pltpu.VMEM((rows, slots * span_pad), f32),
            pltpu.VMEM((rows, HD), f32),
            pltpu.VMEM((rows, HD), f32),
            pltpu.VMEM((slots, rows, HD + kv_cols), bf16),
            pltpu.VMEM((slots, rows, 2 * HD), f32),
            pltpu.VMEM((rows, width), bf16),
            pltpu.VMEM((sections, rows // sections, width), bf16),
            pltpu.VMEM((rows // sections, width), bf16),
            dma((3, slots)),
            dma((2,)),
            each,
            each,
            each,
            each,
            each,
            each,
            each,
            each,
            each,
            each,
            each,
            each,
            each,
            dma((sections,)),
            dma,
        ],
        compiler_params=pltpu.CompilerParams(
            collective_id=0, has_side_effects=True, vmem_limit_bytes=56 * 1024 * 1024
        ),
        name="decode_stack",
    )(*args)


def pick(slots, sections, *args):
    hidden, gain, wq, bias, wkv = args[:5]
    fits = (
        wq.shape[2] == HD
        and wkv.shape[2] % HD == 0
        and slots % KVH == 0
        and sections > 1
        and slots > 1
        and hidden.shape[0] % sections == 0
    )
    return fused_shards(slots, sections, *args) if fits else shards(*args)


def solution(mesh):
    return jax.shard_map(
        functools.partial(pick, mesh.shape["tensor"], mesh.shape["section"]),
        mesh=mesh,
        in_specs=(
            P("groups", "tensor"),
            P("section", None),
            P("section", None, "tensor"),
            P("section", "tensor"),
            P("section", None, "tensor"),
            P("section", None, "tensor"),
            P("section", ("groups", "tensor"), None, None),
            P(("groups", "tensor"), None),
            P(("groups", "tensor")),
        ),
        out_specs=P(("groups", "section"), "tensor"),
        check_vma=False,
    )
```

```python
import functools

import jax
import jax.numpy as jnp
from jax import lax
from jax.experimental import pallas as pl
from jax.experimental.pallas import tpu as pltpu
from jax.sharding import PartitionSpec as P

HD = 128
KVH = 4


epsilon = 1e-06
rope_base = 1000000.0


def shifted(value, axis, steps):
    count = lax.axis_size(axis)
    initial, last = (max(0, -steps), min(count, count - steps))
    return lax.ppermute(value, axis, [(source, source + steps) for source in range(initial, last)])


def rotate(values, position):
    head_size = values.shape[-1]
    half_size = head_size // 2
    frequency = rope_base ** (-(jnp.arange(half_size, dtype=jnp.float32) * 2.0) / head_size)
    angles = position.astype(jnp.float32)[:, None] * frequency[None, :]
    cosine = jnp.cos(angles)[:, None, :]
    sine_part = jnp.sin(angles)[:, None, :]
    front_half = values[..., :half_size]
    back_half = values[..., half_size:]
    return jnp.concatenate(
        [front_half * cosine - back_half * sine_part, back_half * cosine + front_half * sine_part],
        axis=-1,
    )


def attend(queries, key_new, value_new, cached, position):
    row_count, head_count, head_size = queries.shape
    kv_heads = key_new.shape[1]
    group_size = head_count // kv_heads
    span_len = cached.shape[1]
    keys_all = cached[:, :, : kv_heads * head_size].reshape(
        row_count, span_len, kv_heads, head_size
    )
    values_all = cached[:, :, kv_heads * head_size :].reshape(
        row_count, span_len, kv_heads, head_size
    )
    grouped = queries.reshape(row_count, kv_heads, group_size, head_size)
    scaling = head_size ** (-0.5)
    scores = (
        jnp.einsum("rkgd,rskd->rkgs", grouped, keys_all, preferred_element_type=jnp.float32)
        * scaling
    )
    own_score = (
        jnp.einsum("rkgd,rkd->rkg", grouped, key_new, preferred_element_type=jnp.float32) * scaling
    )
    usable = (jnp.arange(span_len, dtype=jnp.int32)[None, :] < position[:, None])[:, None, None, :]
    row_max = jnp.maximum(jnp.max(jnp.where(usable, scores, -1e30), axis=-1), own_score)
    weights = jnp.where(usable, jnp.exp(scores - row_max[..., None]), 0.0)
    own_weight = jnp.exp(own_score - row_max)
    denominator = jnp.sum(weights, axis=-1) + own_weight
    weights = (weights / denominator[..., None]).astype(jnp.bfloat16)
    own_weight = (own_weight / denominator).astype(jnp.bfloat16)
    mixture = jnp.einsum("rkgs,rskd->rkgd", weights, values_all, preferred_element_type=jnp.float32)
    mixture = (
        mixture
        + own_weight.astype(jnp.float32)[..., None] * value_new.astype(jnp.float32)[:, :, None, :]
    )
    return mixture.reshape(row_count, head_count * head_size).astype(jnp.bfloat16)


def shards(
    hidden,
    norm_gain,
    query_weight,
    query_bias,
    kv_weight,
    out_weight,
    kv_pool,
    page_table,
    context_len,
):
    slot_count = lax.axis_size("tensor")
    section_count = lax.axis_size("section")
    section_id = lax.axis_index("section")
    tensor_id = lax.axis_index("tensor")
    row_total, width_dev = hidden.shape
    row_dev = row_total // slot_count
    pool_pages = kv_pool.shape[1]
    gain_row = norm_gain[0].astype(jnp.float32)
    query_proj = query_weight[0]
    bias_row = query_bias[0].astype(jnp.float32)
    kv_proj = kv_weight[0]
    out_proj = out_weight[0]
    pool_layer = kv_pool[0]
    local_pages = page_table - tensor_id * pool_pages
    pieces = 1
    per_piece = row_dev // pieces
    tick_count = section_count + pieces - 1
    is_first = section_id == 0
    finished = [None] * pieces
    carried = jnp.zeros((slot_count * per_piece, width_dev), jnp.bfloat16)
    for tick_index in range(tick_count):
        if tick_index < pieces:
            blocks = hidden.reshape(slot_count, row_dev, hidden.shape[1])
            carried = jnp.where(
                is_first, blocks.reshape(slot_count * per_piece, hidden.shape[1]), carried
            )
        whole = lax.all_gather(carried, "tensor", axis=1, tiled=True)
        wide_rows = whole.astype(jnp.float32)
        mean_sq = jnp.mean(wide_rows * wide_rows, axis=1, keepdims=True)
        normed = (wide_rows * lax.rsqrt(mean_sq + epsilon) * gain_row).astype(jnp.bfloat16)
        queries = (
            jnp.dot(normed, query_proj, preferred_element_type=jnp.float32) + bias_row
        ).astype(jnp.bfloat16)
        fresh_kv = jnp.dot(normed, kv_proj, preferred_element_type=jnp.float32).astype(jnp.bfloat16)
        query_rows = lax.all_to_all(queries, "tensor", split_axis=0, concat_axis=1, tiled=True)
        fresh_rows = lax.all_to_all(fresh_kv, "tensor", split_axis=0, concat_axis=1, tiled=True)
        cached = pool_layer[local_pages].reshape(per_piece, -1, pool_layer.shape[-1])
        rotated = rotate(
            query_rows.reshape(per_piece, -1, HD).astype(jnp.float32), context_len
        ).astype(jnp.bfloat16)
        key_new = rotate(
            fresh_rows[:, : KVH * HD].reshape(per_piece, KVH, HD).astype(jnp.float32), context_len
        ).astype(jnp.bfloat16)
        value_new = fresh_rows[:, KVH * HD :].reshape(per_piece, KVH, HD)
        mixture = attend(rotated, key_new, value_new, cached, context_len)
        carried = (
            carried.astype(jnp.float32)
            + jnp.dot(
                lax.all_gather(mixture, "tensor", axis=0, tiled=True),
                out_proj,
                preferred_element_type=jnp.float32,
            )
        ).astype(jnp.bfloat16)
        if tick_index >= section_count - 1:
            finished[tick_index - section_count + 1] = carried
        if tick_index < tick_count - 1:
            carried = shifted(carried, "section", 1)
    stacked = jnp.concatenate(
        [done_part.reshape(slot_count, per_piece, width_dev) for done_part in finished], axis=1
    )
    result = stacked.reshape(row_total, width_dev)
    is_last = section_id == section_count - 1
    outgoing = jnp.where(is_last, result, jnp.zeros_like(result))[None]
    spread = lax.all_to_all(outgoing, "section", split_axis=1, concat_axis=0, tiled=True)
    return spread[section_count - 1]


MESH = pl.DeviceIdType.MESH
ANY = pl.BlockSpec(memory_space=pl.ANY)
VMEM = pl.BlockSpec(memory_space=pltpu.VMEM)


def fused(
    slots,
    sections,
    hidden,
    gain_in,
    wq,
    bias_in,
    wkv,
    wo,
    pool_in,
    table_in,
    lens_in,
    out,
    gain,
    bias,
    pool,
    table,
    lens,
    wq_v,
    wkv_v,
    wo_v,
    stream,
    keys,
    values,
    meta,
    counts,
    cos_v,
    sin_v,
    fresh,
    parts,
    sent,
    fin,
    fin_in,
    w_sem,
    pool_sem,
    st_send,
    st_recv,
    nx_send,
    key_send,
    key_recv,
    val_send,
    val_recv,
    meta_send,
    meta_recv,
    fresh_send,
    fresh_recv,
    part_send,
    part_recv,
    fin_send,
    fin_recv,
    small_sem,
    go_sem,
):
    f32, bf16 = jnp.float32, jnp.bfloat16
    me = lax.axis_index("tensor")
    sec = lax.axis_index("section")
    rows, width = hidden.shape
    row_dev, blocks = table.shape
    pages, page_len = pool.shape[:2]
    span = pages * page_len
    span_pad = keys.shape[1] * page_len
    kv_cols = wkv.shape[2]
    kv_half = KVH * HD
    group = slots // KVH
    last = sections - 1
    others = range(1, slots)

    ranked = [sorted(range(slots), key=lambda t: abs(t - m)) for m in range(slots)]
    near = [
        sum((me == m).astype(jnp.int32) * ranked[m][k] for m in range(slots))
        for k in range(slots)
    ]

    def peer(k):
        return near[k]

    barrier = pltpu.get_barrier_semaphore()

    def greet(slot, section):
        pl.semaphore_signal(
            barrier,
            inc=1,
            device_id={"tensor": slot, "section": section},
            device_id_type=MESH,
        )

    for k in others:
        greet(peer(k), sec)

    @pl.when(sec > 0)
    def _():
        for t in range(slots):
            greet(t, sec - 1)

    @pl.when(sec < last)
    def _():
        greet(me, last)

    def chunk(ref, src):
        return ref.at[pl.ds(pl.multiple_of(src * width, width), width)]

    def weight_copies(src):
        return (
            pltpu.make_async_copy(chunk(wq.at[0], src), chunk(wq_v, src), w_sem.at[0, src]),
            pltpu.make_async_copy(chunk(wkv.at[0], src), chunk(wkv_v, src), w_sem.at[1, src]),
        )

    def remote(src, dst, send, recv, slot, section):
        return pltpu.make_async_remote_copy(
            src_ref=src,
            dst_ref=dst,
            send_sem=send,
            recv_sem=recv,
            device_id={"tensor": slot, "section": section},
            device_id_type=MESH,
        )

    hidden_copy = pltpu.make_async_copy(hidden, stream.at[me], small_sem.at[0])
    table_copy = pltpu.make_async_copy(table_in, table, small_sem.at[1])
    lens_copy = pltpu.make_async_copy(lens_in, lens, small_sem.at[2])
    gain_copy = pltpu.make_async_copy(gain_in, gain, small_sem.at[3])
    bias_copy = pltpu.make_async_copy(bias_in, bias, small_sem.at[4])
    pool_copy = pltpu.make_async_copy(pool_in.at[0], pool, small_sem.at[5])

    @pl.when(sec == 0)
    def _():
        hidden_copy.start()

    for copy in (table_copy, lens_copy, pool_copy, gain_copy, bias_copy):
        copy.start()
    for k in range(slots):
        for copy in weight_copies(peer(k)):
            copy.start()
    wo_copy = pltpu.make_async_copy(wo.at[0], wo_v, w_sem.at[2, 0])
    wo_copy.start()

    table_copy.wait()
    lens_copy.wait()
    lane = lax.broadcasted_iota(jnp.int32, (row_dev, span_pad), 1)
    row = lax.broadcasted_iota(jnp.int32, (row_dev, span_pad), 0)
    row_c = lax.broadcasted_iota(jnp.int32, (row_dev, HD), 0)
    count = jnp.zeros((row_dev, span_pad), f32)
    length = jnp.zeros((row_dev, HD), f32)
    for r in range(row_dev):
        for b in range(blocks):
            off = lane - (table[r, b] - me * pages) * page_len
            used = (off >= 0) & (off < page_len) & (off + b * page_len < lens[r]) & (row == r)
            count += jnp.where(used, 1.0, 0.0)
        length = jnp.where(row_c == r, lens[r].astype(f32), length)
    meta[me, :, :span_pad] = count
    meta[me, :, span_pad:] = length
    for ref in (keys, values):
        if span_pad > span:
            ref[:, pages:] = jnp.zeros((slots, span_pad // page_len - pages, page_len, HD), bf16)

    pl.semaphore_wait(barrier, 2 * slots - 1 + (last - slots) * (sec // last))

    def first_copies():
        return [
            remote(stream.at[me], stream.at[me], st_send.at[d], st_recv.at[me], peer(d), sec)
            for d in reversed(others)
        ]

    @pl.when(sec == 0)
    def _():
        hidden_copy.wait()
        for copy in first_copies():
            copy.start()

    def pool_part(slot, base):
        first = pl.multiple_of(base + (slot // group) * HD, HD)
        return pool.at[:, :, pl.ds(first, HD)]

    meta_copies, pool_copies = [], []
    for d in others:
        slot = peer(d)
        meta_copies.append(
            remote(meta.at[me], meta.at[me], meta_send.at[d], meta_recv.at[me], slot, sec)
        )
        pool_copies.append(
            remote(
                pool_part(slot, 0),
                keys.at[me, pl.ds(0, pages)],
                key_send.at[d],
                key_recv.at[me],
                slot,
                sec,
            )
        )
        pool_copies.append(
            remote(
                pool_part(slot, kv_half),
                values.at[me, pl.ds(0, pages)],
                val_send.at[d],
                val_recv.at[me],
                slot,
                sec,
            )
        )
    own_pool = [
        pltpu.make_async_copy(pool_part(me, 0), keys.at[me, pl.ds(0, pages)], pool_sem.at[0]),
        pltpu.make_async_copy(
            pool_part(me, kv_half), values.at[me, pl.ds(0, pages)], pool_sem.at[1]
        ),
    ]
    for copy in meta_copies:
        copy.start()

    @pl.when(sec == 0)
    def _():
        for copy in first_copies():
            copy.wait_send()

    @pl.when(sec > 0)
    def _():
        pl.semaphore_wait(go_sem, 1)

    pool_copy.wait()
    for copy in pool_copies + own_pool:
        copy.start()

    def arrived(dst, recv):
        remote(dst, dst, fin_send.at[0], recv, me, lax.rem(sec + 1, sections)).wait_recv()

    for d in others:
        src = peer(d)
        arrived(meta.at[src], meta_recv.at[src])
    counts[...] = jnp.zeros(counts.shape, f32)
    for t in range(slots):
        lines = slice(t * row_dev, (t + 1) * row_dev)
        counts[lines, t * span_pad : (t + 1) * span_pad] = meta[t, :, :span_pad]
        cos_v[lines, :] = meta[t, :, span_pad:]
    spot = lax.broadcasted_iota(jnp.int32, (rows, HD), 1)
    half = HD // 2
    pair = jnp.where(spot < half, spot, spot - half).astype(f32)
    frequency = jnp.exp(pair * (-2.0 / HD) * jnp.log(jnp.full((rows, HD), rope_base, f32)))
    angle = cos_v[...] * frequency
    cosine = jnp.cos(angle)
    sine = jnp.sin(angle) * jnp.where(spot < half, -1.0, 1.0)
    cos_v[...] = cosine
    sin_v[...] = sine

    def rope(x):
        x = x.astype(f32)
        return (x * cos_v[...] + pltpu.roll(x, half, 1) * sin_v[...]).astype(bf16)

    square = jnp.zeros((rows, 1), f32)
    q_sum = jnp.zeros((rows, HD), f32)
    kv_sum = jnp.zeros((rows, kv_cols), f32)
    gain_copy.wait()
    bias_copy.wait()
    for d in range(slots):
        src = peer(d)
        for copy in weight_copies(src):
            copy.wait()
        if d == 0:

            @pl.when(sec > 0)
            def _():
                arrived(stream.at[me], st_recv.at[me])

        else:
            arrived(stream.at[src], st_recv.at[src])
        start = pl.multiple_of(src * width, width)
        x = stream[src].astype(f32)
        square += jnp.sum(x * x, axis=1, keepdims=True)
        scaled = (x * gain[:, pl.ds(start, width)].astype(f32)).astype(bf16)
        q_sum += jnp.dot(scaled, wq_v[pl.ds(start, width), :], preferred_element_type=f32)
        kv_sum += jnp.dot(scaled, wkv_v[pl.ds(start, width), :], preferred_element_type=f32)
    inverse = lax.rsqrt(square * (1.0 / (slots * width)) + epsilon)
    query = rope((q_sum * inverse + bias[...].astype(f32)).astype(bf16))
    kv_new = (kv_sum * inverse).astype(bf16)
    fresh[me, :, :HD] = query
    for j in range(kv_cols // HD):
        piece = kv_new[:, j * HD : (j + 1) * HD]
        is_key = me * kv_cols + j * HD < kv_half
        fresh[me, :, (j + 1) * HD : (j + 2) * HD] = jnp.where(
            is_key, rope(piece).astype(f32), piece.astype(f32)
        ).astype(bf16)
    fresh_copies = [
        remote(fresh.at[me], fresh.at[me], fresh_send.at[d], fresh_recv.at[me], peer(d), sec)
        for d in reversed(others)
    ]
    for copy in fresh_copies:
        copy.start()

    for copy in own_pool:
        copy.wait()
    for d in others:
        src = peer(d)
        arrived(keys.at[src, pl.ds(0, pages)], key_recv.at[src])
        arrived(values.at[src, pl.ds(0, pages)], val_recv.at[src])

    @pl.when(sec < last)
    def _():
        pl.semaphore_signal(
            go_sem, inc=1, device_id={"tensor": me, "section": sec + 1}, device_id_type=MESH
        )

    scaling = HD**-0.5
    times = counts[...]
    scores = (
        lax.dot_general(
            query,
            keys[...].reshape(slots * span_pad, HD),
            (((1,), (1,)), ((), ())),
            preferred_element_type=f32,
        )
        * scaling
    )
    top = jnp.max(jnp.where(times > 0, scores, -1e30), axis=1, keepdims=True)
    weights = jnp.where(times > 0, times * jnp.exp(scores - top), 0.0)
    total = jnp.sum(weights, axis=1, keepdims=True)
    mixed = jnp.dot(
        weights.astype(bf16),
        values[...].reshape(slots * span_pad, HD),
        preferred_element_type=f32,
    )
    parts[me, :, :HD] = mixed / total
    parts[me, :, HD:] = jnp.broadcast_to(top + jnp.log(total), (rows, HD))
    part_copies = [
        remote(parts.at[me], parts.at[me], part_send.at[d], part_recv.at[me], peer(d), sec)
        for d in reversed(others)
    ]
    for copy in part_copies:
        copy.start()

    for d in others:
        src = peer(d)
        arrived(fresh.at[src], fresh_recv.at[src])

    def fresh_head(column):
        first = pl.multiple_of(HD + lax.rem(column, kv_cols), HD)
        return fresh[column // kv_cols, :, pl.ds(first, HD)].astype(f32)

    own, fresh_values = [], []
    for k in range(slots):
        h = peer(k)
        key = fresh_head((h // group) * HD)
        own.append(
            jnp.sum(fresh[h, :, :HD].astype(f32) * key, axis=1, keepdims=True) * scaling
        )
        fresh_values.append(fresh_head(kv_half + (h // group) * HD))
    wo_copy.wait()
    summed = stream[me].astype(f32)
    for k in range(slots):
        h = peer(k)
        if k:
            arrived(parts.at[h], part_recv.at[h])
        share = 1.0 / (1.0 + jnp.exp(parts[h, :, HD:] - own[k]))
        mixture = (parts[h, :, :HD] * (1.0 - share) + fresh_values[k] * share).astype(bf16)
        lines = pl.ds(pl.multiple_of(h * HD, HD), HD)
        summed += jnp.dot(mixture, wo_v[lines, :], preferred_element_type=f32)
    new = summed.astype(bf16)

    def next_copies():
        return [
            remote(sent, stream.at[me], nx_send.at[d], st_recv.at[me], peer(d), sec + 1)
            for d in reversed(range(slots))
        ]

    def fin_copy(j):
        return remote(fin.at[j], fin_in, fin_send.at[j], fin_recv, me, j)

    @pl.when(sec < last)
    def _():
        sent[...] = new
        for copy in next_copies():
            copy.start()
        arrived(fin_in, fin_recv)
        out[...] = fin_in[...]
        for copy in next_copies():
            copy.wait_send()

    @pl.when(sec == last)
    def _():
        out_rows = rows // sections
        wide = new.astype(f32)
        for j in range(last):
            fin[j] = wide[j * out_rows : (j + 1) * out_rows].astype(bf16)
            fin_copy(j).start()
        out[...] = wide[last * out_rows :].astype(bf16)
        for j in range(last):
            fin_copy(j).wait_send()

    for copy in meta_copies + pool_copies + fresh_copies + part_copies:
        copy.wait_send()


def fused_shards(slots, sections, *args):
    hidden, gain, wq, bias, wkv, wo, pool, table, lens = args
    rows, width = hidden.shape
    row_dev = table.shape[0]
    pages, page_len = pool.shape[1:3]
    span_pad = -(-pages * page_len // HD) * HD
    pages_pad = span_pad // page_len
    kv_cols = wkv.shape[2]
    bf16, f32 = jnp.bfloat16, jnp.float32
    dma = pltpu.SemaphoreType.DMA
    each = dma((slots,))
    return pl.pallas_call(
        functools.partial(fused, slots, sections),
        out_shape=jax.ShapeDtypeStruct((rows // sections, width), bf16),
        in_specs=[ANY] * 9,
        out_specs=VMEM,
        scratch_shapes=[
            pltpu.VMEM(gain.shape, bf16),
            pltpu.VMEM(bias.shape, bf16),
            pltpu.VMEM(pool.shape[1:], bf16),
            pltpu.SMEM(table.shape, jnp.int32),
            pltpu.SMEM(lens.shape, jnp.int32),
            pltpu.VMEM(wq.shape[1:], bf16),
            pltpu.VMEM(wkv.shape[1:], bf16),
            pltpu.VMEM(wo.shape[1:], bf16),
            pltpu.VMEM((slots, rows, width), bf16),
            pltpu.VMEM((slots, pages_pad, page_len, HD), bf16),
            pltpu.VMEM((slots, pages_pad, page_len, HD), bf16),
            pltpu.VMEM((slots, row_dev, span_pad + HD), f32),
            pltpu.VMEM((rows, slots * span_pad), f32),
            pltpu.VMEM((rows, HD), f32),
            pltpu.VMEM((rows, HD), f32),
            pltpu.VMEM((slots, rows, HD + kv_cols), bf16),
            pltpu.VMEM((slots, rows, 2 * HD), f32),
            pltpu.VMEM((rows, width), bf16),
            pltpu.VMEM((sections, rows // sections, width), bf16),
            pltpu.VMEM((rows // sections, width), bf16),
            dma((3, slots)),
            dma((2,)),
            each,
            each,
            each,
            each,
            each,
            each,
            each,
            each,
            each,
            each,
            each,
            each,
            each,
            dma((sections,)),
            dma,
            dma((6,)),
            pltpu.SemaphoreType.REGULAR,
        ],
        compiler_params=pltpu.CompilerParams(
            collective_id=0, has_side_effects=True, vmem_limit_bytes=56 * 1024 * 1024
        ),
        name="decode_stack",
    )(*args)


def pick(slots, sections, *args):
    hidden, gain, wq, bias, wkv = args[:5]
    fits = (
        wq.shape[2] == HD
        and wkv.shape[2] % HD == 0
        and slots % KVH == 0
        and sections > 1
        and slots > 1
        and hidden.shape[0] % sections == 0
    )
    return fused_shards(slots, sections, *args) if fits else shards(*args)


def solution(mesh):
    return jax.shard_map(
        functools.partial(pick, mesh.shape["tensor"], mesh.shape["section"]),
        mesh=mesh,
        in_specs=(
            P("groups", "tensor"),
            P("section", None),
            P("section", None, "tensor"),
            P("section", "tensor"),
            P("section", None, "tensor"),
            P("section", None, "tensor"),
            P("section", ("groups", "tensor"), None, None),
            P(("groups", "tensor"), None),
            P(("groups", "tensor")),
        ),
        out_specs=P(("groups", "section"), "tensor"),
        check_vma=False,
    )
```

```python
import functools

import jax
import jax.numpy as jnp
from jax import lax
from jax.experimental import pallas as pl
from jax.experimental.pallas import tpu as pltpu
from jax.sharding import PartitionSpec as P

HD = 128
KVH = 4


epsilon = 1e-06
rope_base = 1000000.0


def shifted(value, axis, steps):
    count = lax.axis_size(axis)
    initial, last = (max(0, -steps), min(count, count - steps))
    return lax.ppermute(value, axis, [(source, source + steps) for source in range(initial, last)])


def rotate(values, position):
    head_size = values.shape[-1]
    half_size = head_size // 2
    frequency = rope_base ** (-(jnp.arange(half_size, dtype=jnp.float32) * 2.0) / head_size)
    angles = position.astype(jnp.float32)[:, None] * frequency[None, :]
    cosine = jnp.cos(angles)[:, None, :]
    sine_part = jnp.sin(angles)[:, None, :]
    front_half = values[..., :half_size]
    back_half = values[..., half_size:]
    return jnp.concatenate(
        [front_half * cosine - back_half * sine_part, back_half * cosine + front_half * sine_part],
        axis=-1,
    )


def attend(queries, key_new, value_new, cached, position):
    row_count, head_count, head_size = queries.shape
    kv_heads = key_new.shape[1]
    group_size = head_count // kv_heads
    span_len = cached.shape[1]
    keys_all = cached[:, :, : kv_heads * head_size].reshape(
        row_count, span_len, kv_heads, head_size
    )
    values_all = cached[:, :, kv_heads * head_size :].reshape(
        row_count, span_len, kv_heads, head_size
    )
    grouped = queries.reshape(row_count, kv_heads, group_size, head_size)
    scaling = head_size ** (-0.5)
    scores = (
        jnp.einsum("rkgd,rskd->rkgs", grouped, keys_all, preferred_element_type=jnp.float32)
        * scaling
    )
    own_score = (
        jnp.einsum("rkgd,rkd->rkg", grouped, key_new, preferred_element_type=jnp.float32) * scaling
    )
    usable = (jnp.arange(span_len, dtype=jnp.int32)[None, :] < position[:, None])[:, None, None, :]
    row_max = jnp.maximum(jnp.max(jnp.where(usable, scores, -1e30), axis=-1), own_score)
    weights = jnp.where(usable, jnp.exp(scores - row_max[..., None]), 0.0)
    own_weight = jnp.exp(own_score - row_max)
    denominator = jnp.sum(weights, axis=-1) + own_weight
    weights = (weights / denominator[..., None]).astype(jnp.bfloat16)
    own_weight = (own_weight / denominator).astype(jnp.bfloat16)
    mixture = jnp.einsum("rkgs,rskd->rkgd", weights, values_all, preferred_element_type=jnp.float32)
    mixture = (
        mixture
        + own_weight.astype(jnp.float32)[..., None] * value_new.astype(jnp.float32)[:, :, None, :]
    )
    return mixture.reshape(row_count, head_count * head_size).astype(jnp.bfloat16)


def shards(
    hidden,
    norm_gain,
    query_weight,
    query_bias,
    kv_weight,
    out_weight,
    kv_pool,
    page_table,
    context_len,
):
    slot_count = lax.axis_size("tensor")
    section_count = lax.axis_size("section")
    section_id = lax.axis_index("section")
    tensor_id = lax.axis_index("tensor")
    row_total, width_dev = hidden.shape
    row_dev = row_total // slot_count
    pool_pages = kv_pool.shape[1]
    gain_row = norm_gain[0].astype(jnp.float32)
    query_proj = query_weight[0]
    bias_row = query_bias[0].astype(jnp.float32)
    kv_proj = kv_weight[0]
    out_proj = out_weight[0]
    pool_layer = kv_pool[0]
    local_pages = page_table - tensor_id * pool_pages
    pieces = 1
    per_piece = row_dev // pieces
    tick_count = section_count + pieces - 1
    is_first = section_id == 0
    finished = [None] * pieces
    carried = jnp.zeros((slot_count * per_piece, width_dev), jnp.bfloat16)
    for tick_index in range(tick_count):
        if tick_index < pieces:
            blocks = hidden.reshape(slot_count, row_dev, hidden.shape[1])
            carried = jnp.where(
                is_first, blocks.reshape(slot_count * per_piece, hidden.shape[1]), carried
            )
        whole = lax.all_gather(carried, "tensor", axis=1, tiled=True)
        wide_rows = whole.astype(jnp.float32)
        mean_sq = jnp.mean(wide_rows * wide_rows, axis=1, keepdims=True)
        normed = (wide_rows * lax.rsqrt(mean_sq + epsilon) * gain_row).astype(jnp.bfloat16)
        queries = (
            jnp.dot(normed, query_proj, preferred_element_type=jnp.float32) + bias_row
        ).astype(jnp.bfloat16)
        fresh_kv = jnp.dot(normed, kv_proj, preferred_element_type=jnp.float32).astype(jnp.bfloat16)
        query_rows = lax.all_to_all(queries, "tensor", split_axis=0, concat_axis=1, tiled=True)
        fresh_rows = lax.all_to_all(fresh_kv, "tensor", split_axis=0, concat_axis=1, tiled=True)
        cached = pool_layer[local_pages].reshape(per_piece, -1, pool_layer.shape[-1])
        rotated = rotate(
            query_rows.reshape(per_piece, -1, HD).astype(jnp.float32), context_len
        ).astype(jnp.bfloat16)
        key_new = rotate(
            fresh_rows[:, : KVH * HD].reshape(per_piece, KVH, HD).astype(jnp.float32), context_len
        ).astype(jnp.bfloat16)
        value_new = fresh_rows[:, KVH * HD :].reshape(per_piece, KVH, HD)
        mixture = attend(rotated, key_new, value_new, cached, context_len)
        carried = (
            carried.astype(jnp.float32)
            + jnp.dot(
                lax.all_gather(mixture, "tensor", axis=0, tiled=True),
                out_proj,
                preferred_element_type=jnp.float32,
            )
        ).astype(jnp.bfloat16)
        if tick_index >= section_count - 1:
            finished[tick_index - section_count + 1] = carried
        if tick_index < tick_count - 1:
            carried = shifted(carried, "section", 1)
    stacked = jnp.concatenate(
        [done_part.reshape(slot_count, per_piece, width_dev) for done_part in finished], axis=1
    )
    result = stacked.reshape(row_total, width_dev)
    is_last = section_id == section_count - 1
    outgoing = jnp.where(is_last, result, jnp.zeros_like(result))[None]
    spread = lax.all_to_all(outgoing, "section", split_axis=1, concat_axis=0, tiled=True)
    return spread[section_count - 1]


MESH = pl.DeviceIdType.MESH
HBM = pl.BlockSpec(memory_space=pltpu.HBM)
VMEM = pl.BlockSpec(memory_space=pltpu.VMEM)


def fused(
    slots,
    sections,
    hidden,
    gain_in,
    wq,
    bias_in,
    wkv,
    wo,
    pool_in,
    table_in,
    lens_in,
    out,
    gain,
    bias,
    pool,
    table,
    lens,
    wq_v,
    wkv_v,
    wo_v,
    stream,
    keys,
    values,
    meta,
    counts,
    cos_v,
    sin_v,
    fresh,
    parts,
    sent,
    fin,
    fin_in,
    w_sem,
    pool_sem,
    st_send,
    st_recv,
    nx_send,
    key_send,
    key_recv,
    val_send,
    val_recv,
    meta_send,
    meta_recv,
    fresh_send,
    fresh_recv,
    part_send,
    part_recv,
    fin_send,
    fin_recv,
    small_sem,
    go_sem,
):
    f32, bf16 = jnp.float32, jnp.bfloat16
    me = lax.axis_index("tensor")
    sec = lax.axis_index("section")
    rows, width = hidden.shape
    row_dev, blocks = table.shape
    pages, page_len = pool.shape[:2]
    span = pages * page_len
    span_pad = keys.shape[1] * page_len
    kv_cols = wkv.shape[2]
    kv_half = KVH * HD
    group = slots // KVH
    last = sections - 1
    others = range(1, slots)

    ranked = [
        sorted(range(slots), key=lambda t: (abs(t - m), t // 2 != m // 2)) for m in range(slots)
    ]
    near = [
        sum((me == m).astype(jnp.int32) * ranked[m][k] for m in range(slots))
        for k in range(slots)
    ]

    def peer(k):
        return near[k]

    barrier = pltpu.get_barrier_semaphore()

    def greet(slot, section):
        pl.semaphore_signal(
            barrier,
            inc=1,
            device_id={"tensor": slot, "section": section},
            device_id_type=MESH,
        )

    for k in others:
        greet(peer(k), sec)

    @pl.when(sec > 0)
    def _():
        for t in range(slots):
            greet(t, sec - 1)

    @pl.when(sec < last)
    def _():
        greet(me, last)

    def chunk(ref, src):
        return ref.at[pl.ds(pl.multiple_of(src * width, width), width)]

    def weight_copies(src):
        return (
            pltpu.make_async_copy(chunk(wq.at[0], src), chunk(wq_v, src), w_sem.at[0, src]),
            pltpu.make_async_copy(chunk(wkv.at[0], src), chunk(wkv_v, src), w_sem.at[1, src]),
        )

    def remote(src, dst, send, recv, slot, section):
        return pltpu.make_async_remote_copy(
            src_ref=src,
            dst_ref=dst,
            send_sem=send,
            recv_sem=recv,
            device_id={"tensor": slot, "section": section},
            device_id_type=MESH,
        )

    hidden_copy = pltpu.make_async_copy(hidden, stream.at[me], small_sem.at[0])
    table_copy = pltpu.make_async_copy(table_in, table, small_sem.at[1])
    lens_copy = pltpu.make_async_copy(lens_in, lens, small_sem.at[2])
    gain_copy = pltpu.make_async_copy(gain_in, gain, small_sem.at[3])
    bias_copy = pltpu.make_async_copy(bias_in, bias, small_sem.at[4])
    pool_copy = pltpu.make_async_copy(pool_in.at[0], pool, small_sem.at[5])

    @pl.when(sec == 0)
    def _():
        hidden_copy.start()

    for copy in (table_copy, lens_copy, pool_copy, gain_copy, bias_copy):
        copy.start()
    for k in range(slots):
        for copy in weight_copies(peer(k)):
            copy.start()
    wo_copy = pltpu.make_async_copy(wo.at[0], wo_v, w_sem.at[2, 0])
    wo_copy.start()

    pl.semaphore_wait(barrier, 2 * slots - 1 + (last - slots) * (sec // last))

    def first_copies():
        return [
            remote(stream.at[me], stream.at[me], st_send.at[d], st_recv.at[me], peer(d), sec)
            for d in reversed(others)
        ]

    @pl.when(sec == 0)
    def _():
        hidden_copy.wait()
        for copy in first_copies():
            copy.start()

    table_copy.wait()
    lens_copy.wait()
    lane = lax.broadcasted_iota(jnp.int32, (row_dev, span_pad), 1)
    row = lax.broadcasted_iota(jnp.int32, (row_dev, span_pad), 0)
    row_c = lax.broadcasted_iota(jnp.int32, (row_dev, HD), 0)
    count = jnp.zeros((row_dev, span_pad), f32)
    length = jnp.zeros((row_dev, HD), f32)
    for r in range(row_dev):
        for b in range(blocks):
            off = lane - (table[r, b] - me * pages) * page_len
            used = (off >= 0) & (off < page_len) & (off + b * page_len < lens[r]) & (row == r)
            count += jnp.where(used, 1.0, 0.0)
        length = jnp.where(row_c == r, lens[r].astype(f32), length)
    meta[me, :, :span_pad] = count
    meta[me, :, span_pad:] = length

    for ref in (keys, values):
        if span_pad > span:
            ref[:, pages:] = jnp.zeros((slots, span_pad // page_len - pages, page_len, HD), bf16)

    def pool_part(slot, base):
        first = pl.multiple_of(base + (slot // group) * HD, HD)
        return pool.at[:, :, pl.ds(first, HD)]

    meta_copies, pool_copies, value_copies = [], [], []
    for d in others:
        slot = peer(d)
        meta_copies.append(
            remote(meta.at[me], meta.at[me], meta_send.at[d], meta_recv.at[me], slot, sec)
        )
        pool_copies.append(
            remote(
                pool_part(slot, 0),
                keys.at[me, pl.ds(0, pages)],
                key_send.at[d],
                key_recv.at[me],
                slot,
                sec,
            )
        )
        value_copies.append(
            remote(
                pool_part(slot, kv_half),
                values.at[me, pl.ds(0, pages)],
                val_send.at[d],
                val_recv.at[me],
                slot,
                sec,
            )
        )
    own_pool = [
        pltpu.make_async_copy(pool_part(me, 0), keys.at[me, pl.ds(0, pages)], pool_sem.at[0]),
        pltpu.make_async_copy(
            pool_part(me, kv_half), values.at[me, pl.ds(0, pages)], pool_sem.at[1]
        ),
    ]
    for copy in meta_copies:
        copy.start()

    @pl.when(sec == 1)
    def _():
        pl.semaphore_wait(go_sem, 1)

    pool_copy.wait()
    pool_copies += value_copies
    for copy in own_pool + pool_copies:
        copy.start()

    def arrived(dst, recv):
        remote(dst, dst, fin_send.at[0], recv, me, lax.rem(sec + 1, sections)).wait_recv()

    half = HD // 2

    def tables():
        for d in others:
            src = peer(d)
            arrived(meta.at[src], meta_recv.at[src])
        counts[...] = jnp.zeros(counts.shape, f32)
        for t in range(slots):
            lines = slice(t * row_dev, (t + 1) * row_dev)
            counts[lines, t * span_pad : (t + 1) * span_pad] = meta[t, :, :span_pad]
            cos_v[lines, :] = meta[t, :, span_pad:]
        spot = lax.broadcasted_iota(jnp.int32, (rows, HD), 1)
        pair = jnp.where(spot < half, spot, spot - half).astype(f32)
        frequency = jnp.exp(pair * (-2.0 / HD) * jnp.log(jnp.full((rows, HD), rope_base, f32)))
        angle = cos_v[...] * frequency
        cosine = jnp.cos(angle)
        sine = jnp.sin(angle) * jnp.where(spot < half, -1.0, 1.0)
        cos_v[...] = cosine
        sin_v[...] = sine

    pl.when(sec > 0)(tables)

    def rope(x):
        x = x.astype(f32)
        return (x * cos_v[...] + pltpu.roll(x, half, 1) * sin_v[...]).astype(bf16)

    square = jnp.zeros((rows, 1), f32)
    q_sum = jnp.zeros((rows, HD), f32)
    kv_sum = jnp.zeros((rows, kv_cols), f32)
    gain_copy.wait()
    bias_copy.wait()
    for d in range(slots):
        src = peer(d)
        for copy in weight_copies(src):
            copy.wait()
        if d == 0:

            @pl.when(sec > 0)
            def _():
                arrived(stream.at[me], st_recv.at[me])

        else:
            arrived(stream.at[src], st_recv.at[src])
        if d == 1:

            @pl.when(sec == 0)
            def _():
                pl.semaphore_signal(
                    go_sem, inc=1, device_id={"tensor": me, "section": 1}, device_id_type=MESH
                )

        start = pl.multiple_of(src * width, width)
        x = stream[src].astype(f32)
        square += jnp.sum(x * x, axis=1, keepdims=True)
        scaled = (x * gain[:, pl.ds(start, width)].astype(f32)).astype(bf16)
        q_sum += jnp.dot(scaled, wq_v[pl.ds(start, width), :], preferred_element_type=f32)
        kv_sum += jnp.dot(scaled, wkv_v[pl.ds(start, width), :], preferred_element_type=f32)
    pl.when(sec == 0)(tables)
    inverse = lax.rsqrt(square * (1.0 / (slots * width)) + epsilon)
    query = rope((q_sum * inverse + bias[...].astype(f32)).astype(bf16))
    kv_new = (kv_sum * inverse).astype(bf16)
    fresh[me, :, :HD] = query
    for j in range(kv_cols // HD):
        piece = kv_new[:, j * HD : (j + 1) * HD]
        is_key = me * kv_cols + j * HD < kv_half
        fresh[me, :, (j + 1) * HD : (j + 2) * HD] = jnp.where(
            is_key, rope(piece).astype(f32), piece.astype(f32)
        ).astype(bf16)
    fresh_copies = [
        remote(fresh.at[me], fresh.at[me], fresh_send.at[d], fresh_recv.at[me], peer(d), sec)
        for d in reversed(others)
    ]
    for copy in fresh_copies:
        copy.start()

    own_pool[0].wait()
    for d in others:
        src = peer(d)
        arrived(keys.at[src, pl.ds(0, pages)], key_recv.at[src])
    scaling = HD**-0.5
    times = counts[...]
    scores = (
        lax.dot_general(
            query,
            keys[...].reshape(slots * span_pad, HD),
            (((1,), (1,)), ((), ())),
            preferred_element_type=f32,
        )
        * scaling
    )
    top = jnp.max(jnp.where(times > 0, scores, -1e30), axis=1, keepdims=True)
    weights = jnp.where(times > 0, times * jnp.exp(scores - top), 0.0)
    total = jnp.sum(weights, axis=1, keepdims=True)
    own_pool[1].wait()
    for d in others:
        src = peer(d)
        arrived(values.at[src, pl.ds(0, pages)], val_recv.at[src])
    mixed = jnp.dot(
        weights.astype(bf16),
        values[...].reshape(slots * span_pad, HD),
        preferred_element_type=f32,
    )
    parts[me, :, :HD] = mixed / total
    parts[me, :, HD:] = jnp.broadcast_to(top + jnp.log(total), (rows, HD))
    part_copies = [
        remote(parts.at[me], parts.at[me], part_send.at[d], part_recv.at[me], peer(d), sec)
        for d in reversed(others)
    ]
    for copy in part_copies:
        copy.start()

    def fresh_head(column):
        first = pl.multiple_of(HD + lax.rem(column, kv_cols), HD)
        return fresh[column // kv_cols, :, pl.ds(first, HD)].astype(f32)

    reach = [
        max(
            ranked[m].index(t)
            for m in range(slots)
            for h in [ranked[m][k]]
            for column in [(h // group) * HD]
            for t in [h, column // kv_cols, (kv_half + column) // kv_cols]
        )
        for k in range(slots)
    ]
    summed = stream[me].astype(f32)
    wo_copy.wait()
    near_by = 0
    for k in range(slots):
        h = peer(k)
        while near_by < reach[k]:
            near_by += 1
            arrived(fresh.at[peer(near_by)], fresh_recv.at[peer(near_by)])
        key = fresh_head((h // group) * HD)
        value = fresh_head(kv_half + (h // group) * HD)
        own = jnp.sum(fresh[h, :, :HD].astype(f32) * key, axis=1, keepdims=True) * scaling
        if k:
            arrived(parts.at[h], part_recv.at[h])
        share = 1.0 / (1.0 + jnp.exp(parts[h, :, HD:] - own))
        mixture = (parts[h, :, :HD] * (1.0 - share) + value * share).astype(bf16)
        lines = pl.ds(pl.multiple_of(h * HD, HD), HD)
        summed += jnp.dot(mixture, wo_v[lines, :], preferred_element_type=f32)
    while near_by < slots - 1:
        near_by += 1
        arrived(fresh.at[peer(near_by)], fresh_recv.at[peer(near_by)])
    new = summed.astype(bf16)

    def next_copies():
        return [
            remote(sent, stream.at[me], nx_send.at[d], st_recv.at[me], peer(d), sec + 1)
            for d in reversed(range(slots))
        ]

    def fin_copy(j):
        return remote(fin.at[j], fin_in, fin_send.at[j], fin_recv, me, j)

    @pl.when(sec < last)
    def _():
        sent[...] = new
        for copy in next_copies():
            copy.start()
        arrived(fin_in, fin_recv)
        out[...] = fin_in[...]
        for copy in next_copies():
            copy.wait_send()

    @pl.when(sec == last)
    def _():
        out_rows = rows // sections
        wide = new.astype(f32)
        for j in range(last):
            fin[j] = wide[j * out_rows : (j + 1) * out_rows].astype(bf16)
            fin_copy(j).start()
        out[...] = wide[last * out_rows :].astype(bf16)
        for j in range(last):
            fin_copy(j).wait_send()

    @pl.when(sec == 0)
    def _():
        for copy in first_copies():
            copy.wait_send()

    for copy in meta_copies + pool_copies + fresh_copies + part_copies:
        copy.wait_send()


def fused_shards(slots, sections, *args):
    hidden, gain, wq, bias, wkv, wo, pool, table, lens = args
    rows, width = hidden.shape
    row_dev = table.shape[0]
    pages, page_len = pool.shape[1:3]
    span_pad = -(-pages * page_len // HD) * HD
    pages_pad = span_pad // page_len
    kv_cols = wkv.shape[2]
    bf16, f32 = jnp.bfloat16, jnp.float32
    dma = pltpu.SemaphoreType.DMA
    each = dma((slots,))
    return pl.pallas_call(
        functools.partial(fused, slots, sections),
        out_shape=jax.ShapeDtypeStruct((rows // sections, width), bf16),
        in_specs=[HBM] * 9,
        out_specs=VMEM,
        scratch_shapes=[
            pltpu.VMEM(gain.shape, bf16),
            pltpu.VMEM(bias.shape, bf16),
            pltpu.VMEM(pool.shape[1:], bf16),
            pltpu.SMEM(table.shape, jnp.int32),
            pltpu.SMEM(lens.shape, jnp.int32),
            pltpu.VMEM(wq.shape[1:], bf16),
            pltpu.VMEM(wkv.shape[1:], bf16),
            pltpu.VMEM(wo.shape[1:], bf16),
            pltpu.VMEM((slots, rows, width), bf16),
            pltpu.VMEM((slots, pages_pad, page_len, HD), bf16),
            pltpu.VMEM((slots, pages_pad, page_len, HD), bf16),
            pltpu.VMEM((slots, row_dev, span_pad + HD), f32),
            pltpu.VMEM((rows, slots * span_pad), f32),
            pltpu.VMEM((rows, HD), f32),
            pltpu.VMEM((rows, HD), f32),
            pltpu.VMEM((slots, rows, HD + kv_cols), bf16),
            pltpu.VMEM((slots, rows, 2 * HD), f32),
            pltpu.VMEM((rows, width), bf16),
            pltpu.VMEM((sections, rows // sections, width), bf16),
            pltpu.VMEM((rows // sections, width), bf16),
            dma((3, slots)),
            dma((2,)),
            each,
            each,
            each,
            each,
            each,
            each,
            each,
            each,
            each,
            each,
            each,
            each,
            each,
            dma((sections,)),
            dma,
            dma((6,)),
            pltpu.SemaphoreType.REGULAR,
        ],
        compiler_params=pltpu.CompilerParams(
            collective_id=0, has_side_effects=True, vmem_limit_bytes=56 * 1024 * 1024
        ),
        name="decode_stack",
    )(*args)


def pick(slots, sections, *args):
    hidden, gain, wq, bias, wkv = args[:5]
    fits = (
        wq.shape[2] == HD
        and wkv.shape[2] % HD == 0
        and slots % KVH == 0
        and sections > 1
        and slots > 1
        and hidden.shape[0] % sections == 0
    )
    return fused_shards(slots, sections, *args) if fits else shards(*args)


def solution(mesh):
    return jax.shard_map(
        functools.partial(pick, mesh.shape["tensor"], mesh.shape["section"]),
        mesh=mesh,
        in_specs=(
            P("groups", "tensor"),
            P("section", None),
            P("section", None, "tensor"),
            P("section", "tensor"),
            P("section", None, "tensor"),
            P("section", None, "tensor"),
            P("section", ("groups", "tensor"), None, None),
            P(("groups", "tensor"), None),
            P(("groups", "tensor")),
        ),
        out_specs=P(("groups", "section"), "tensor"),
        check_vma=False,
    )
```
